32 devices in a mesh: dp: 2 (over z, core), sp: 16 (over x, y).
Axes of the slice: x: 4, y: 4, z: 1, core: 2. Of those that a mesh axis runs over, the one named last changes fastest.
The devices are a block of a 4x4x8 slice.
Arguments:
- x: bfloat16 [16384, 2048], P(('dp', 'sp')), parts along dimension 0
- gain: bfloat16 [2048], replicated
- wq: bfloat16 [2048, 2048], P('sp')
- wk: bfloat16 [2048, 256], P('sp')
- wv: bfloat16 [2048, 256], P('sp')
- wo: bfloat16 [2048, 2048], P('sp')
Outputs:
- output: bfloat16 [16384, 2048], P(('dp', 'sp')), parts along dimension 0
There are 2 independent parts. The reference program is written for one: setup_inputs(seed, part) draws one part's arguments, and reference() takes and returns one part's arrays. A program takes and returns all parts, laid end to end along the dimension named above; an argument that names none is the same for every part.
All inputs are finite; a program needn't handle non-finite values.
Results may differ from the reference program's by a relative error of at most 0.012.
Values are sent between devices in bfloat16 or wider.
A program may use at most 768 MiB of HBM per device.

```python
import jax
import jax.numpy as jnp
from jax import lax

ROWS = 8192
D = 2048
HEADS = 8
KV_HEADS = 1
HEAD = 256
THETA = 10000


def setup_inputs(seed: int = 0, part: int = 0) -> dict:
    kx, kn, kq, kk, kv, ko = jax.random.split(jax.random.key(seed), 6)

    def weights(key, rows, columns):
        return jax.random.normal(key, (rows, columns), jnp.float32) * rows**-0.5

    drawn = {
        "x": jax.random.normal(jax.random.fold_in(kx, part), (ROWS, D), jnp.float32),
        "gain": 1 + 0.1 * jax.random.normal(kn, (D,), jnp.float32),
        "wq": 2 * weights(kq, D, HEADS * HEAD),
        "wk": 2 * weights(kk, D, KV_HEADS * HEAD),
        "wv": 4 * weights(kv, D, KV_HEADS * HEAD),
        "wo": weights(ko, HEADS * HEAD, D),
    }
    return {k: v.astype(jnp.bfloat16) for k, v in drawn.items()}


def normed(x, gain):
    wide = x.astype(jnp.float32)
    scale = lax.rsqrt(jnp.mean(wide * wide, -1, keepdims=True) + 1e-6)
    return (wide * scale * gain.astype(jnp.float32)).astype(jnp.bfloat16)


def turned(t, place, theta):
    half = t.shape[-1] // 2
    angle = place.astype(jnp.float32)[:, None] * theta ** (-jnp.arange(half, dtype=jnp.float32) / half)
    cos, sin = jnp.cos(angle)[:, None], jnp.sin(angle)[:, None]
    a, b = t[..., :half].astype(jnp.float32), t[..., half:].astype(jnp.float32)
    return jnp.concatenate([a * cos - b * sin, b * cos + a * sin], -1).astype(jnp.bfloat16)


def matmul(a, w):
    return jnp.dot(a, w, preferred_element_type=jnp.float32).astype(jnp.bfloat16)


def einsum(form, a, b):
    return jnp.einsum(form, a.astype(jnp.float32), b.astype(jnp.float32))


def attention(q, k, v):
    scores = einsum("tgsd,ugd->gstu", q, k) * q.shape[-1] ** -0.5
    token = jnp.arange(q.shape[0])
    scores = jnp.where(token[:, None] >= token, scores, -jnp.inf)
    weights = jax.nn.softmax(scores, -1).astype(jnp.bfloat16)
    return einsum("gstu,ugd->tgsd", weights, v).astype(jnp.bfloat16)


def reference(x, gain, wq, wk, wv, wo):
    a, place = normed(x, gain), jnp.arange(ROWS)
    q = turned(matmul(a, wq).reshape(ROWS, HEADS, HEAD), place, THETA).reshape(ROWS, KV_HEADS, -1, HEAD)
    k = turned(matmul(a, wk).reshape(ROWS, KV_HEADS, HEAD), place, THETA)
    v = matmul(a, wv).reshape(ROWS, KV_HEADS, HEAD)
    seen = attention(q, k, v).reshape(ROWS, HEADS * HEAD)
    return (x.astype(jnp.float32) + jnp.dot(seen, wo, preferred_element_type=jnp.float32)).astype(jnp.bfloat16)
```

```python
import functools
import math

import jax
import jax.numpy as jnp
from jax import lax
from jax.experimental import pallas as pl
from jax.experimental.pallas import tpu as pltpu
from jax.sharding import PartitionSpec as P

HEAD = 256
THETA = 10000
NEG = -1e30
HIDDEN = 2 * NEG
LOG2E = 1.4426950408889634
VMEM = 67_043_328
MESH = pl.DeviceIdType.MESH


def _dot(a, b, ca, cb):
    return lax.dot_general(a, b, (((ca,), (cb,)), ((), ())), preferred_element_type=jnp.float32)


def _gray(i):
    return i + (i // 2) * (1 - 2 * (i % 2))


def _kernel(side, x_hbm, gain_ref, freq_ref, wq_hbm, wk_hbm, wv_hbm, wo_hbm, y_hbm, x_s, a_s, w_s, wo_s, k_s, vt_s, qt_s, mix_s, top_s, cos_s,
            sin_s, y_s, local_sem, w_recv, wo_recv, kv_recv, pair_recv, send_sem, pair_send, y_sem):
    n = side * side
    own, dim = x_hbm.shape
    shard = wq_hbm.shape[0]
    part, chunk = shard // 2, shard // 4
    qd = wq_hbm.shape[1]
    heads = qd // HEAD
    half = HEAD // 2
    e = HEAD**-0.5 * LOG2E

    me = lax.axis_index("sp")
    group = lax.axis_index("dp")
    odd = group % 2
    partner = group + 1 - 2 * odd
    px, py = me // side, me % side
    first = px * (1 - odd) + py * odd
    second = py * (1 - odd) + px * odd

    def place(f, s):
        f, s = (f + side) % side, (s + side) % side
        return (f * (1 - odd) + s * odd) * side + s * (1 - odd) + f * odd

    def source(df, ds):
        return place(first - df, second - ds)

    up1, down1 = place(first + 1, second), place(first - 1, second)
    up2, down2 = place(first, second + 1), place(first, second - 1)

    def w_chunk(ref):
        def at(src, c):
            return ref.at[pl.ds(pl.multiple_of(src * shard + odd * part + c * chunk, chunk), chunk), :]

        return at

    def kv_chunk(src, c):
        return k_s.at[pl.ds(pl.multiple_of(src * own, own), own), :] if c == 0 else vt_s.at[src]

    gathers = {"w": (w_chunk(w_s), w_recv, 0), "wo": (w_chunk(wo_s), wo_recv, 2), "kv": (kv_chunk, kv_recv, 4)}

    def send(name, src, c, target, df, ds):
        at, recv, sem = gathers[name]
        pltpu.make_async_remote_copy(at(src, c), at(src, c), send_sem.at[sem + c], recv.at[df * side + ds, c], device_id={"sp": target},
                                     device_id_type=MESH).start()

    def start(name):
        for c in range(2):
            send(name, me, c, up1, 1, 0)
            send(name, me, c, down1, side - 1, 0)
            send(name, me, c, up2, 0, 1)
            send(name, me, c, down2, 0, side - 1)

    def pair_copy(ref, src, i):
        rows = ref.at[pl.ds(pl.multiple_of(src * shard + odd * part, part), part), :]
        return pltpu.make_async_remote_copy(rows, rows, pair_send.at[i], pair_recv.at[i], device_id={"dp": partner}, device_id_type=MESH)

    def relay(name, t):
        df, ds = _gray(t % side), _gray(t // side)
        src = source(df, ds)
        at, recv, sem = gathers[name]
        for c in range(2):
            pltpu.make_async_remote_copy(at(src, c), at(src, c), send_sem.at[sem + c], recv.at[df * side + ds, c], device_id={"sp": up1},
                                         device_id_type=MESH).wait_recv()
            turn, on1, on2 = (1, up1, up2) if c == 0 else (side - 1, down1, down2)

            @pl.when(ds == 0)
            def _():
                @pl.when(df == turn)
                def _():
                    send(name, src, c, on1, 2, 0)

                send(name, src, c, up2, df, 1)
                send(name, src, c, down2, df, side - 1)

            @pl.when(ds == turn)
            def _():
                send(name, src, c, on2, df, 2)

        if name != "kv":
            pair_copy(w_s if name == "w" else wo_s, src, 0 if name == "w" else 1).start()
        return src

    def pair_wait(ref, i):
        rows = ref.at[pl.ds(0, (n - 1) * part), :]
        return pltpu.make_async_remote_copy(rows, rows, pair_send.at[i], pair_recv.at[i], device_id={"dp": partner}, device_id_type=MESH)

    mine = pl.ds(pl.multiple_of(me * shard, shard), shard)
    kd = wk_hbm.shape[1]
    copies = [
        pltpu.make_async_copy(wq_hbm, w_s.at[mine, pl.ds(0, qd)], local_sem.at[0]),
        pltpu.make_async_copy(wk_hbm, w_s.at[mine, pl.ds(qd, kd)], local_sem.at[1]),
        pltpu.make_async_copy(wv_hbm, w_s.at[mine, pl.ds(qd + kd, kd)], local_sem.at[2]),
        pltpu.make_async_copy(x_hbm, x_s, local_sem.at[3]),
        pltpu.make_async_copy(wo_hbm, wo_s.at[mine, :], local_sem.at[4]),
    ]
    for copy in copies:
        copy.start()

    barrier = pltpu.get_barrier_semaphore()
    for target in (up1, down1, up2, down2):
        pl.semaphore_signal(barrier, inc=1, device_id={"sp": target}, device_id_type=MESH)
    pl.semaphore_signal(barrier, inc=1, device_id={"dp": partner}, device_id_type=MESH)
    for copy in copies[:3]:
        copy.wait()
    pl.semaphore_wait(barrier, 5)
    start("w")

    copies[3].wait()
    rows = 128

    def norm(i, _):
        here = pl.ds(pl.multiple_of(i * rows, rows), rows)
        wide = x_s[here, :].astype(jnp.float32)
        scale = lax.rsqrt(jnp.mean(wide * wide, -1, keepdims=True) + 1e-6)
        a_s[here, :] = (wide * scale * gain_ref[...].astype(jnp.float32)).astype(jnp.bfloat16)

    lax.fori_loop(0, own // rows, norm, None)
    where = (me * own + lax.broadcasted_iota(jnp.int32, (own, half), 0)).astype(jnp.float32)
    angle = where * freq_ref[...]
    cos_s[...] = jnp.cos(angle)
    sin_s[...] = jnp.sin(angle)
    top_s[...] = jnp.full(top_s.shape, NEG, jnp.float32)
    mix_s[...] = jnp.zeros(mix_s.shape, jnp.float32)

    lax.fori_loop(1, n, lambda t, _: (relay("w", t), None)[1], None)
    pair_wait(w_s, 0).wait_recv()

    def project(at):
        return _dot(a_s[...], w_s[:, pl.ds(pl.multiple_of(at, HEAD), HEAD)], 1, 0).astype(jnp.bfloat16)

    def turned(t):
        a, b = t[:, :half].astype(jnp.float32), t[:, half:].astype(jnp.float32)
        cos, sin = cos_s[...], sin_s[...]
        return jnp.concatenate([a * cos - b * sin, b * cos + a * sin], -1)

    k_s[pl.ds(pl.multiple_of(me * own, own), own), :] = turned(project(qd)).astype(jnp.bfloat16)
    vt_s[me] = project(qd + kd).astype(jnp.float32).T.astype(jnp.bfloat16)

    def query(h):
        qt_s[:, pl.ds(pl.multiple_of(h * own, own), own)] = turned(project(h * HEAD)).T.astype(jnp.bfloat16)

    query(0)
    start("kv")
    lax.fori_loop(1, heads, lambda h, _: query(h), None)

    ones = jnp.ones((8, own), jnp.bfloat16)

    def block(j, masked):
        keys = k_s[pl.ds(pl.multiple_of(j * own, own), own), :]
        scores = [_dot(keys, qt_s[:, h * own : (h + 1) * own], 1, 0) for h in range(heads)]
        if masked:
            ok = lax.broadcasted_iota(jnp.int32, (own, own), 1) >= lax.broadcasted_iota(jnp.int32, (own, own), 0)
        weights, keeps = [], []
        for h, s in enumerate(scores):
            here = slice(h * own, (h + 1) * own)
            if masked:
                s = jnp.where(ok, s, HIDDEN)
            old = top_s[:, here]
            top = jnp.maximum(old, s.max(axis=0, keepdims=True))
            top_s[:, here] = top
            weights.append(jnp.exp2((s - top) * e).astype(jnp.bfloat16))
            keeps.append(jnp.exp2((old - top) * e))
        for h, (p, keep) in enumerate(zip(weights, keeps)):
            here = slice(h * own, (h + 1) * own)
            values = jnp.concatenate([vt_s[j], ones], axis=0)
            mix_s[:, here] = mix_s[:, here] * keep + _dot(values, p, 1, 0)

    block(me, True)
    copies[4].wait()

    def attend(t, _):
        src = relay("kv", t)

        @pl.when(t == 1)
        def _():
            start("wo")

        @pl.when(t >= 4)
        def _():
            relay("wo", t - 3)

        @pl.when(src < me)
        def _():
            block(src, False)

    lax.fori_loop(1, n, attend, None)

    for h in range(heads):
        here = slice(h * own, (h + 1) * own)
        a_s[:, h * HEAD : (h + 1) * HEAD] = (mix_s[:HEAD, here] * (1 / mix_s[HEAD : HEAD + 1, here])).T.astype(jnp.bfloat16)

    lax.fori_loop(n - 3, n, lambda t, _: (relay("wo", t), None)[1], None)
    pair_wait(wo_s, 1).wait_recv()

    wide = 512
    outs = []
    for i in range(dim // wide):
        here = slice(i * wide, (i + 1) * wide)
        got = _dot(a_s[...], wo_s[:, here], 1, 0)
        y_s[:, here] = (x_s[:, here].astype(jnp.float32) + got).astype(jnp.bfloat16)
        outs.append(pltpu.make_async_copy(y_s.at[:, pl.ds(i * wide, wide)], y_hbm.at[:, pl.ds(i * wide, wide)], y_sem.at[i]))
        outs[-1].start()

    for name, ref in (("w", w_s), ("wo", wo_s)):
        for c in range(2):
            rows = ref.at[pl.ds(0, (n - 1) * chunk), :]
            pltpu.make_async_remote_copy(rows, rows, send_sem.at[gathers[name][2] + c], w_recv.at[0, 0], device_id={"sp": up1},
                                         device_id_type=MESH).wait_send()
    rows = k_s.at[pl.ds(0, (n - 1) * own), :]
    pltpu.make_async_remote_copy(rows, rows, send_sem.at[4], w_recv.at[0, 0], device_id={"sp": up1}, device_id_type=MESH).wait_send()
    rows = vt_s.at[pl.ds(0, n - 1)]
    pltpu.make_async_remote_copy(rows, rows, send_sem.at[5], w_recv.at[0, 0], device_id={"sp": up1}, device_id_type=MESH).wait_send()
    pair_wait(w_s, 0).wait_send()
    pair_wait(wo_s, 1).wait_send()
    for out in outs:
        out.wait()


def solution(mesh):
    n = mesh.shape["sp"]
    side = math.isqrt(n)

    def step(x, gain, wq, wk, wv, wo):
        own, dim = x.shape
        shard, qd = wq.shape
        kd = wk.shape[1]
        heads, half = qd // HEAD, HEAD // 2
        freq = (THETA ** (-jnp.arange(half, dtype=jnp.float32) / half))[None]
        low, wide = jnp.bfloat16, jnp.float32
        dma = pltpu.SemaphoreType.DMA
        anywhere, vmem = pl.BlockSpec(memory_space=pl.ANY), pl.BlockSpec(memory_space=pltpu.VMEM)
        return pl.pallas_call(
            functools.partial(_kernel, side),
            out_shape=jax.ShapeDtypeStruct((own, dim), low),
            in_specs=[anywhere, vmem, vmem, anywhere, anywhere, anywhere, anywhere],
            out_specs=anywhere,
            scratch_shapes=[
                pltpu.VMEM((own, dim), low),
                pltpu.VMEM((own, dim), low),
                pltpu.VMEM((n * shard, qd + 2 * kd), low),
                pltpu.VMEM((n * wo.shape[0], wo.shape[1]), low),
                pltpu.VMEM((n * own, HEAD), low),
                pltpu.VMEM((n, HEAD, own), low),
                pltpu.VMEM((HEAD, heads * own), low),
                pltpu.VMEM((HEAD + 8, heads * own), wide),
                pltpu.VMEM((1, heads * own), wide),
                pltpu.VMEM((own, half), wide),
                pltpu.VMEM((own, half), wide),
                pltpu.VMEM((own, dim), low),
                dma((5,)),
                dma((n, 2)),
                dma((n, 2)),
                dma((n, 2)),
                dma((2,)),
                dma((6,)),
                dma((2,)),
                dma((dim // 512,)),
            ],
            compiler_params=pltpu.CompilerParams(collective_id=0, has_side_effects=True, vmem_limit_bytes=VMEM),
        )(x, gain[None], freq, wq, wk, wv, wo)

    tokens, whole = P(("dp", "sp"), None), P("sp", None)
    return jax.shard_map(
        step,
        mesh=mesh,
        in_specs=(tokens, P(None), whole, whole, whole, whole),
        out_specs=tokens,
        check_vma=False,
    )
```

```python
import functools
import math

import jax
import jax.numpy as jnp
import numpy as np
from jax import lax
from jax.experimental import pallas as pl
from jax.experimental.pallas import tpu as pltpu
from jax.sharding import PartitionSpec as P

HEAD = 256
THETA = 10000
NEG = -1e30
HIDDEN = 2 * NEG
LOG2E = 1.4426950408889634
VMEM = 67_043_328
EARLY = 9
AHEAD = 0
AHEAD_WO = 13
MESH = pl.DeviceIdType.MESH


def _dot(a, b, ca, cb):
    return lax.dot_general(a, b, (((ca,), (cb,)), ((), ())), preferred_element_type=jnp.float32)


def _gray(i):
    return i + (i // 2) * (1 - 2 * (i % 2))


def _turn(t):
    near = ((t // 4 + 1) // 2) % 2
    df = _gray(near * ((t + 4) // 2 % 4) + (1 - near) * (t % 4))
    return df, near * (1 + 2 * (t % 2)) + (1 - near) * 2 * (t // 12)


def _kernel(side, x_hbm, gain_ref, freq_ref, wq_hbm, wk_hbm, wv_hbm, wo_hbm, y_ref, x_s, a_s, w_s, wo_s, k_s, vt_s, qt_s, mix_s, top_s, cos_s,
            sin_s, early_s, local_sem, w_recv, wo_recv, kv_recv, pair_recv, send_sem, pair_send):
    n = side * side
    own, dim = x_hbm.shape
    shard = wq_hbm.shape[0]
    part, chunk = shard // 2, shard // 4
    qd = wq_hbm.shape[1]
    heads = qd // HEAD
    half = HEAD // 2
    e = HEAD**-0.5 * LOG2E

    me = lax.axis_index("sp")
    group = lax.axis_index("dp")
    odd = group % 2
    partner = group + 1 - 2 * odd
    px, py = me // side, me % side
    first = px * (1 - odd) + py * odd
    second = py * (1 - odd) + px * odd

    def place(f, s):
        f, s = (f + side) % side, (s + side) % side
        return (f * (1 - odd) + s * odd) * side + s * (1 - odd) + f * odd

    def source(df, ds):
        return place(first - df, second - ds)

    up1, down1 = place(first + 1, second), place(first - 1, second)
    up2, down2 = place(first, second + 1), place(first, second - 1)

    def slot(df, ds):
        dx, dy = df * (1 - odd) + ds * odd, ds * (1 - odd) + df * odd
        fx, fy = (dx // 2) * (1 - dx % 2), (dy // 2) * (1 - dy % 2)
        gx, gy = dx - dx // 2, dy - dy // 2
        return (1 - fx) * ((1 - fy) * (gx * (side - 1) + gy) + fy * (EARLY + side + gx)) + fx * (EARLY + dy)

    def w_chunk(src, c, df, ds):
        return w_s.at[pl.ds(pl.multiple_of(slot(df, ds) * shard + odd * part + c * chunk, chunk), chunk), :]

    def wo_chunk(src, c, df, ds):
        return wo_s.at[pl.ds(pl.multiple_of(slot(df, ds) * shard + odd * part + c * chunk, chunk), chunk), :]

    def kv_chunk(src, c, df, ds):
        return k_s.at[pl.ds(pl.multiple_of(src * own, own), own), :] if c == 0 else vt_s.at[src]

    gathers = {"w": (w_chunk, w_recv, 0), "wo": (wo_chunk, wo_recv, 2), "kv": (kv_chunk, kv_recv, 4)}

    def send(name, src, c, target, here, there):
        at, recv, sem = gathers[name]
        df, ds = there
        pltpu.make_async_remote_copy(at(src, c, *here), at(src, c, df, ds), send_sem.at[sem + c], recv.at[df * side + ds, c],
                                     device_id={"sp": target}, device_id_type=MESH).start()

    def start_first(name):
        for c in range(2):
            send(name, me, c, up1, (0, 0), (1, 0))
            send(name, me, c, down1, (0, 0), (side - 1, 0))

    def start_second(name):
        for c in range(2):
            send(name, me, c, up2, (0, 0), (0, 1))
            send(name, me, c, down2, (0, 0), (0, side - 1))

    def pair_copy(rows, i):
        return pltpu.make_async_remote_copy(rows, rows, pair_send.at[i], pair_recv.at[i], device_id={"dp": partner}, device_id_type=MESH)

    def pair_w(ref, place, i):
        return pair_copy(ref.at[pl.ds(pl.multiple_of(place * shard + odd * part, part), part), :], i)

    def pair_all(ref, blocks, i):
        return pair_copy(ref.at[pl.ds(0, blocks * part), :], i)

    def relay(name, t):
        df, ds = here = _turn(t)
        src = source(df, ds)
        at, recv, sem = gathers[name]
        for c in range(2):
            ref = at(src, c, df, ds)
            pltpu.make_async_remote_copy(ref, ref, send_sem.at[sem + c], recv.at[df * side + ds, c], device_id={"sp": up1},
                                         device_id_type=MESH).wait_recv()
            turn, on1, on2 = (1, up1, up2) if c == 0 else (side - 1, down1, down2)

            @pl.when(ds == 0)
            def _():
                @pl.when(df == turn)
                def _():
                    send(name, src, c, on1, here, (2, 0))

                send(name, src, c, up2, here, (df, 1))
                send(name, src, c, down2, here, (df, side - 1))

            @pl.when(ds == turn)
            def _():
                send(name, src, c, on2, here, (df, 2))

        if name != "kv":
            ref, i = (w_s, 0) if name == "w" else (wo_s, 2)
            far = (df == 2) | (ds == 2)

            @pl.when(far)
            def _():
                pair_w(ref, slot(df, ds), i + 1).start()

            @pl.when(jnp.logical_not(far))
            def _():
                pair_w(ref, slot(df, ds), i).start()

        return src

    top = pl.ds(0, shard)
    kd = wk_hbm.shape[1]
    copies = [
        pltpu.make_async_copy(wq_hbm, w_s.at[top, pl.ds(0, qd)], local_sem.at[0]),
        pltpu.make_async_copy(wk_hbm, w_s.at[top, pl.ds(qd, kd)], local_sem.at[1]),
        pltpu.make_async_copy(wv_hbm, w_s.at[top, pl.ds(qd + kd, kd)], local_sem.at[2]),
        pltpu.make_async_copy(x_hbm, x_s, local_sem.at[3]),
        pltpu.make_async_copy(wo_hbm, wo_s.at[top, :], local_sem.at[4]),
    ]
    for copy in copies[:3]:
        copy.start()

    barrier = pltpu.get_barrier_semaphore()
    for target in (up1, down1, up2, down2):
        pl.semaphore_signal(barrier, inc=1, device_id={"sp": target}, device_id_type=MESH)
    pl.semaphore_signal(barrier, inc=1, device_id={"dp": partner}, device_id_type=MESH)
    for copy in copies[:3]:
        copy.wait()
    pl.semaphore_wait(barrier, 5)
    start_first("w")
    start_second("w")
    for copy in copies[3:]:
        copy.start()
    for t in range(1, side):
        relay("w", t)

    def columns_of(i):
        dx, dy = (px - i // side + side) % side, (py - i % side + side) % side
        return pl.ds(pl.multiple_of(slot(dx * (1 - odd) + dy * odd, dy * (1 - odd) + dx * odd) * shard, shard), shard)

    copies[3].wait()
    gain = gain_ref[...].astype(jnp.float32).reshape(1, dim)
    rows = own // side

    def prepare(t, _):
        relay("w", t)
        at = pl.multiple_of((t - side) * rows, rows)
        here = pl.ds(at, rows)
        wide = x_s[here, :].astype(jnp.float32)
        scale = lax.rsqrt(jnp.mean(wide * wide, -1, keepdims=True) + 1e-6)
        state = (wide * scale * gain).astype(jnp.bfloat16)
        for i in range(n):
            a_s[here, columns_of(i)] = state[:, i * shard : (i + 1) * shard]
        where = (me * own + at + lax.broadcasted_iota(jnp.int32, (rows, half), 0)).astype(jnp.float32)
        angle = where * freq_ref[...]
        cos_s[here, :] = jnp.cos(angle)
        sin_s[here, :] = jnp.sin(angle)

    lax.fori_loop(side, 2 * side, prepare, None)
    top_s[...] = jnp.full(top_s.shape, NEG, jnp.float32)
    mix_s[...] = jnp.zeros(mix_s.shape, jnp.float32)
    lax.fori_loop(2 * side, n - side, lambda t, _: (relay("w", t), None)[1], None)
    copies[4].wait()
    start_first("wo")

    early = EARLY * shard

    def columns(at):
        return pl.ds(pl.multiple_of(at, HEAD), HEAD)

    def project_early(i):
        at = columns(i * HEAD)
        early_s[:, at] = _dot(a_s[:, :early], w_s[:early, at], 1, 0)

    pair_all(w_s, EARLY - 1, 0).wait_recv()
    pieces = (qd + 2 * kd) // HEAD

    def rest(t, _):
        for i in range(-(-pieces // side)):
            at = (t - n + side) * -(-pieces // side) + i

            @pl.when(at < pieces)
            def _():
                project_early(at)

        relay("w", t)

    lax.fori_loop(n - side, n, rest, None)
    pair_all(w_s, n - EARLY, 1).wait_recv()

    def project(at):
        at = columns(at)
        return (early_s[:, at] + _dot(a_s[:, early:], w_s[early:, at], 1, 0)).astype(jnp.bfloat16)

    def turned(t):
        a, b = t[:, :half].astype(jnp.float32), t[:, half:].astype(jnp.float32)
        cos, sin = cos_s[...], sin_s[...]
        return jnp.concatenate([a * cos - b * sin, b * cos + a * sin], -1)

    k_s[pl.ds(pl.multiple_of(me * own, own), own), :] = turned(project(qd)).astype(jnp.bfloat16)
    vt_s[me] = project(qd + kd).astype(jnp.float32).T.astype(jnp.bfloat16)

    def query(h):
        qt_s[:, pl.ds(pl.multiple_of(h * own, own), own)] = turned(project(h * HEAD)).T.astype(jnp.bfloat16)

    query(0)
    start_first("kv")

    lax.fori_loop(1, heads, lambda h, _: query(h), None)
    start_second("kv")

    ones = jnp.ones((8, own), jnp.bfloat16)

    def block(j, masked):
        keys = k_s[pl.ds(pl.multiple_of(j * own, own), own), :]
        values = jnp.concatenate([vt_s[j], ones], axis=0)
        if masked:
            ok = lax.broadcasted_iota(jnp.int32, (own, own), 1) >= lax.broadcasted_iota(jnp.int32, (own, own), 0)

        def score(h):
            return _dot(keys, qt_s[:, h * own : (h + 1) * own], 1, 0)

        def weigh(h, s):
            here = slice(h * own, (h + 1) * own)
            if masked:
                s = jnp.where(ok, s, HIDDEN)
            old = top_s[:, here]
            top = jnp.maximum(old, s.max(axis=0, keepdims=True))
            top_s[:, here] = top
            return jnp.exp2((s - top) * e).astype(jnp.bfloat16), jnp.exp2((old - top) * e)

        def mix(h, p, keep):
            here = slice(h * own, (h + 1) * own)
            mix_s[:, here] = mix_s[:, here] * keep + _dot(values, p, 1, 0)

        scores = [score(0), score(1)]
        last = None
        for h in range(heads):
            if h + 2 < heads:
                scores.append(score(h + 2))
            now = weigh(h, scores[h])
            if last is not None:
                mix(h - 1, *last)
            last = now
        mix(heads - 1, *last)

    block(me, True)
    for t in range(1, AHEAD + 1):
        relay("kv", t)

    def attend(t, _):
        @pl.when(t < n - AHEAD)
        def _():
            relay("kv", t + AHEAD)

        @pl.when(t == side - 1)
        def _():
            start_second("wo")

        @pl.when(t >= n - AHEAD_WO + 1)
        def _():
            relay("wo", t - n + AHEAD_WO)

        src = source(*_turn(t))

        @pl.when(src < me)
        def _():
            block(src, False)

    lax.fori_loop(1, n, attend, None)

    for h in range(heads):
        here = slice(h * own, (h + 1) * own)
        seen = (mix_s[:HEAD, here] * (1 / mix_s[HEAD : HEAD + 1, here])).T.astype(jnp.bfloat16)
        for i in range(HEAD // shard):
            a_s[:, columns_of(h * (HEAD // shard) + i)] = seen[:, i * shard : (i + 1) * shard]

    for t in range(AHEAD_WO, n):
        relay("wo", t)
    pair_all(wo_s, EARLY - 1, 2).wait_recv()
    wide = 512
    for i in range(dim // wide):
        here = slice(i * wide, (i + 1) * wide)
        early_s[:, here] = x_s[:, here].astype(jnp.float32) + _dot(a_s[:, :early], wo_s[:early, here], 1, 0)
    pair_all(wo_s, n - EARLY, 3).wait_recv()
    for i in range(dim // wide):
        here = slice(i * wide, (i + 1) * wide)
        y_ref[:, here] = (early_s[:, here] + _dot(a_s[:, early:], wo_s[early:, here], 1, 0)).astype(jnp.bfloat16)

    for name, ref in (("w", w_s), ("wo", wo_s)):
        for c in range(2):
            rows = ref.at[pl.ds(0, (n - 1) * chunk), :]
            pltpu.make_async_remote_copy(rows, rows, send_sem.at[gathers[name][2] + c], w_recv.at[0, 0], device_id={"sp": up1},
                                         device_id_type=MESH).wait_send()
    rows = k_s.at[pl.ds(0, (n - 1) * own), :]
    pltpu.make_async_remote_copy(rows, rows, send_sem.at[4], w_recv.at[0, 0], device_id={"sp": up1}, device_id_type=MESH).wait_send()
    rows = vt_s.at[pl.ds(0, n - 1)]
    pltpu.make_async_remote_copy(rows, rows, send_sem.at[5], w_recv.at[0, 0], device_id={"sp": up1}, device_id_type=MESH).wait_send()
    pair_all(w_s, EARLY - 1, 0).wait_send()
    pair_all(w_s, n - EARLY, 1).wait_send()
    pair_all(wo_s, EARLY - 1, 2).wait_send()
    pair_all(wo_s, n - EARLY, 3).wait_send()


def solution(mesh):
    n = mesh.shape["sp"]
    side = math.isqrt(n)

    def step(x, gain, wq, wk, wv, wo):
        own, dim = x.shape
        shard, qd = wq.shape
        kd = wk.shape[1]
        heads, half = qd // HEAD, HEAD // 2
        freq = jnp.asarray((THETA ** (-np.arange(half) / half))[None].astype(np.float32))
        low, wide = jnp.bfloat16, jnp.float32
        dma = pltpu.SemaphoreType.DMA
        anywhere, vmem = pl.BlockSpec(memory_space=pl.ANY), pl.BlockSpec(memory_space=pltpu.VMEM)
        return pl.pallas_call(
            functools.partial(_kernel, side),
            out_shape=pltpu.VMEM((own, dim), low),
            in_specs=[anywhere, vmem, vmem, anywhere, anywhere, anywhere, anywhere],
            out_specs=vmem,
            scratch_shapes=[
                pltpu.VMEM((own, dim), low),
                pltpu.VMEM((own, dim), low),
                pltpu.VMEM((n * shard, qd + 2 * kd), low),
                pltpu.VMEM((n * wo.shape[0], wo.shape[1]), low),
                pltpu.VMEM((n * own, HEAD), low),
                pltpu.VMEM((n, HEAD, own), low),
                pltpu.VMEM((HEAD, heads * own), low),
                pltpu.VMEM((HEAD + 8, heads * own), wide),
                pltpu.VMEM((1, heads * own), wide),
                pltpu.VMEM((own, half), wide),
                pltpu.VMEM((own, half), wide),
                pltpu.VMEM((own, qd + 2 * kd), wide),
                dma((5,)),
                dma((n, 2)),
                dma((n, 2)),
                dma((n, 2)),
                dma((4,)),
                dma((6,)),
                dma((4,)),
            ],
            compiler_params=pltpu.CompilerParams(collective_id=0, has_side_effects=True, vmem_limit_bytes=VMEM - 2 * own * dim),
        )(x, gain, freq, wq, wk, wv, wo)

    tokens, whole = P(("dp", "sp"), None), P("sp", None)
    return jax.shard_map(
        step,
        mesh=mesh,
        in_specs=(tokens, P(None), whole, whole, whole, whole),
        out_specs=tokens,
        check_vma=False,
    )
```

```python
import functools
import math

import jax
import jax.numpy as jnp
import numpy as np
from jax import lax
from jax.experimental import pallas as pl
from jax.experimental.pallas import tpu as pltpu
from jax.sharding import PartitionSpec as P

HEAD = 256
THETA = 10000
NEG = -1e30
HIDDEN = 2 * NEG
LOG2E = 1.4426950408889634
VMEM = 67_043_328
EARLY = 9
AHEAD = 0
AHEAD_WO = 13
MESH = pl.DeviceIdType.MESH


def _dot(a, b, ca, cb):
    return lax.dot_general(a, b, (((ca,), (cb,)), ((), ())), preferred_element_type=jnp.float32)


def _gray(i):
    return jnp.where(i >= 2, 5 - i, i)


def _turn(t):
    t = jnp.int32(t)
    t = jnp.where((t >= 3) & (t <= 5), jnp.where(t == 5, 3, t + 1), t)
    near = (t >= 4) & (t < 12)
    df = _gray(jnp.where(near, lax.div(t - 4, 2), lax.rem(t, 4)))
    return df, jnp.where(near, 1 + 2 * lax.rem(t, 2), jnp.where(t >= 12, 2, 0))


def _kernel(side, x_hbm, gain_ref, freq_ref, wq_hbm, wk_hbm, wv_hbm, wo_hbm, y_ref, x_s, a_s, w_s, wo_s, k_s, vt_s, qt_s, mix_s, top_s, cos_s,
            sin_s, early_s, local_sem, w_recv, wo_recv, kv_recv, pair_recv, send_sem, pair_send):
    n = side * side
    own, dim = x_hbm.shape
    shard = wq_hbm.shape[0]
    part, chunk = shard // 2, shard // 4
    qd = wq_hbm.shape[1]
    heads = qd // HEAD
    half = HEAD // 2
    e = HEAD**-0.5 * LOG2E

    me = lax.axis_index("sp")
    group = lax.axis_index("dp")
    odd = group % 2
    partner = group + 1 - 2 * odd
    px, py = me // side, me % side
    first = px * (1 - odd) + py * odd
    second = py * (1 - odd) + px * odd

    by_first, by_second = side * (1 - odd) + odd, side * odd + 1 - odd

    def place(f, s):
        f, s = lax.rem(f + side, side), lax.rem(s + side, side)
        return f * by_first + s * by_second

    def source(df, ds):
        return place(first - df, second - ds)

    up1, down1 = place(first + 1, second), place(first - 1, second)
    up2, down2 = place(first, second + 1), place(first, second - 1)

    def slot(df, ds):
        dx, dy = jnp.where(odd == 1, ds, df), jnp.where(odd == 1, df, ds)
        gx, gy = jnp.minimum(dx, 2), jnp.minimum(dy, 2)
        return jnp.where(dx == 2, EARLY + dy, jnp.where(dy == 2, EARLY + side + gx, gx * (side - 1) + gy))

    def w_chunk(src, c, df, ds):
        return w_s.at[pl.ds(pl.multiple_of(slot(df, ds) * shard + odd * part + c * chunk, chunk), chunk), :]

    def wo_chunk(src, c, df, ds):
        return wo_s.at[pl.ds(pl.multiple_of(slot(df, ds) * shard + odd * part + c * chunk, chunk), chunk), :]

    def kv_chunk(src, c, df, ds):
        return k_s.at[pl.ds(pl.multiple_of(src * own, own), own), :] if c == 0 else vt_s.at[src]

    gathers = {"w": (w_chunk, w_recv, 0), "wo": (wo_chunk, wo_recv, 2), "kv": (kv_chunk, kv_recv, 4)}

    def send(name, src, c, target, here, there):
        at, recv, sem = gathers[name]
        df, ds = there
        pltpu.make_async_remote_copy(at(src, c, *here), at(src, c, df, ds), send_sem.at[sem + c], recv.at[df * side + ds, c],
                                     device_id={"sp": target}, device_id_type=MESH).start()

    def start_first(name):
        for c in range(2):
            send(name, me, c, up1, (0, 0), (1, 0))
            send(name, me, c, down1, (0, 0), (side - 1, 0))

    def start_second(name):
        for c in range(2):
            send(name, me, c, up2, (0, 0), (0, 1))
            send(name, me, c, down2, (0, 0), (0, side - 1))

    def pair_copy(rows, i):
        return pltpu.make_async_remote_copy(rows, rows, pair_send.at[i], pair_recv.at[i], device_id={"dp": partner}, device_id_type=MESH)

    def pair_w(ref, place, i):
        return pair_copy(ref.at[pl.ds(pl.multiple_of(place * shard + odd * part, part), part), :], i)

    def pair_all(ref, blocks, i):
        return pair_copy(ref.at[pl.ds(0, blocks * part), :], i)

    def relay(name, t):
        df, ds = here = _turn(t)
        src = source(df, ds)
        at, recv, sem = gathers[name]
        for c in range(2):
            ref = at(src, c, df, ds)
            pltpu.make_async_remote_copy(ref, ref, send_sem.at[sem + c], recv.at[df * side + ds, c], device_id={"sp": up1},
                                         device_id_type=MESH).wait_recv()
            turn, on1, on2 = (1, up1, up2) if c == 0 else (side - 1, down1, down2)

            @pl.when(ds == 0)
            def _():
                @pl.when(df == turn)
                def _():
                    send(name, src, c, on1, here, (2, 0))

                send(name, src, c, up2, here, (df, 1))
                send(name, src, c, down2, here, (df, side - 1))

            @pl.when(ds == turn)
            def _():
                send(name, src, c, on2, here, (df, 2))

        if name != "kv":
            ref, i = (w_s, 0) if name == "w" else (wo_s, 2)
            far = (df == 2) | (ds == 2)

            @pl.when(far)
            def _():
                pair_w(ref, slot(df, ds), i + 1).start()

            @pl.when(jnp.logical_not(far))
            def _():
                pair_w(ref, slot(df, ds), i).start()

        return src

    top = pl.ds(0, shard)
    kd = wk_hbm.shape[1]
    copies = [
        pltpu.make_async_copy(wq_hbm, w_s.at[top, pl.ds(0, qd)], local_sem.at[0]),
        pltpu.make_async_copy(wk_hbm, w_s.at[top, pl.ds(qd, kd)], local_sem.at[1]),
        pltpu.make_async_copy(wv_hbm, w_s.at[top, pl.ds(qd + kd, kd)], local_sem.at[2]),
        pltpu.make_async_copy(x_hbm, x_s, local_sem.at[3]),
        pltpu.make_async_copy(wo_hbm, wo_s.at[top, :], local_sem.at[4]),
    ]
    for copy in copies[:3]:
        copy.start()

    barrier = pltpu.get_barrier_semaphore()
    for target in (up1, down1, up2, down2):
        pl.semaphore_signal(barrier, inc=1, device_id={"sp": target}, device_id_type=MESH)
    pl.semaphore_signal(barrier, inc=1, device_id={"dp": partner}, device_id_type=MESH)
    for copy in copies[:3]:
        copy.wait()
    pl.semaphore_wait(barrier, 5)
    start_first("w")
    start_second("w")
    for copy in copies[3:]:
        copy.start()
    for t in range(1, side):
        relay("w", t)

    def columns_of(i):
        dx, dy = (px - i // side + side) % side, (py - i % side + side) % side
        return pl.ds(pl.multiple_of(slot(dx * (1 - odd) + dy * odd, dy * (1 - odd) + dx * odd) * shard, shard), shard)

    copies[3].wait()
    gain = gain_ref[...].astype(jnp.float32).reshape(1, dim)
    rows = own // side

    def prepare(t, _):
        relay("w", t)
        at = pl.multiple_of((t - side) * rows, rows)
        here = pl.ds(at, rows)
        wide = x_s[here, :].astype(jnp.float32)
        scale = lax.rsqrt(jnp.mean(wide * wide, -1, keepdims=True) + 1e-6)
        state = (wide * scale * gain).astype(jnp.bfloat16)
        for i in range(n):
            a_s[here, columns_of(i)] = state[:, i * shard : (i + 1) * shard]
        where = (me * own + at + lax.broadcasted_iota(jnp.int32, (rows, half), 0)).astype(jnp.float32)
        angle = where * freq_ref[...]
        cos_s[here, :] = jnp.cos(angle)
        sin_s[here, :] = jnp.sin(angle)

    lax.fori_loop(side, 2 * side, prepare, None)
    copies[4].wait()
    start_first("wo")
    start_second("wo")
    top_s[...] = jnp.full(top_s.shape, NEG, jnp.float32)
    mix_s[...] = jnp.zeros(mix_s.shape, jnp.float32)
    lax.fori_loop(2 * side, n - side, lambda t, _: (relay("w", t), None)[1], None)

    early = EARLY * shard

    def columns(at):
        return pl.ds(pl.multiple_of(at, HEAD), HEAD)

    def project_early(i):
        at = columns(i * HEAD)
        early_s[:, at] = _dot(a_s[:, :early], w_s[:early, at], 1, 0)

    pair_all(w_s, EARLY - 1, 0).wait_recv()
    pieces = (qd + 2 * kd) // HEAD

    def rest(t, _):
        for i in range(-(-pieces // side)):
            at = (t - n + side) * -(-pieces // side) + i

            @pl.when(at < pieces)
            def _():
                project_early(at)

        relay("w", t)

    lax.fori_loop(n - side, n, rest, None)
    pair_all(w_s, n - EARLY, 1).wait_recv()

    def project(at):
        at = columns(at)
        return (early_s[:, at] + _dot(a_s[:, early:], w_s[early:, at], 1, 0)).astype(jnp.bfloat16)

    def turned(t):
        a, b = t[:, :half].astype(jnp.float32), t[:, half:].astype(jnp.float32)
        cos, sin = cos_s[...], sin_s[...]
        return jnp.concatenate([a * cos - b * sin, b * cos + a * sin], -1)

    k_s[pl.ds(pl.multiple_of(me * own, own), own), :] = turned(project(qd)).astype(jnp.bfloat16)
    vt_s[me] = project(qd + kd).astype(jnp.float32).T.astype(jnp.bfloat16)

    def query(h):
        qt_s[:, pl.ds(pl.multiple_of(h * own, own), own)] = turned(project(h * HEAD)).T.astype(jnp.bfloat16)

    query(0)
    start_first("kv")

    lax.fori_loop(1, heads, lambda h, _: query(h), None)
    start_second("kv")

    ones = jnp.ones((8, own), jnp.bfloat16)

    def block(j, masked):
        keys = k_s[pl.ds(pl.multiple_of(j * own, own), own), :]
        values = jnp.concatenate([vt_s[j], ones], axis=0)
        if masked:
            ok = lax.broadcasted_iota(jnp.int32, (own, own), 1) >= lax.broadcasted_iota(jnp.int32, (own, own), 0)

        def score(h):
            return _dot(keys, qt_s[:, h * own : (h + 1) * own], 1, 0)

        def weigh(h, s):
            here = slice(h * own, (h + 1) * own)
            if masked:
                s = jnp.where(ok, s, HIDDEN)
            old = top_s[:, here]
            top = jnp.maximum(old, s.max(axis=0, keepdims=True))
            top_s[:, here] = top
            return jnp.exp2((s - top) * e).astype(jnp.bfloat16), jnp.exp2((old - top) * e)

        def mix(h, p, keep):
            here = slice(h * own, (h + 1) * own)
            mix_s[:, here] = mix_s[:, here] * keep + _dot(values, p, 1, 0)

        scores = [score(0), score(1)]
        last = None
        for h in range(heads):
            if h + 2 < heads:
                scores.append(score(h + 2))
            now = weigh(h, scores[h])
            if last is not None:
                mix(h - 1, *last)
            last = now
        mix(heads - 1, *last)

    block(me, True)
    for t in range(1, AHEAD + 1):
        relay("kv", t)

    def attend(t, _):
        @pl.when(t < n - AHEAD)
        def _():
            relay("kv", t + AHEAD)

        @pl.when(t >= n - AHEAD_WO + 1)
        def _():
            relay("wo", t - n + AHEAD_WO)

        src = source(*_turn(t))

        @pl.when(src < me)
        def _():
            block(src, False)

    lax.fori_loop(1, n, attend, None)

    for h in range(heads):
        here = slice(h * own, (h + 1) * own)
        seen = (mix_s[:HEAD, here] * (1 / mix_s[HEAD : HEAD + 1, here])).T.astype(jnp.bfloat16)
        for i in range(HEAD // shard):
            a_s[:, columns_of(h * (HEAD // shard) + i)] = seen[:, i * shard : (i + 1) * shard]

    for t in range(AHEAD_WO, n):
        relay("wo", t)
    pair_all(wo_s, EARLY - 1, 2).wait_recv()
    wide = 512
    for i in range(dim // wide):
        here = slice(i * wide, (i + 1) * wide)
        early_s[:, here] = x_s[:, here].astype(jnp.float32) + _dot(a_s[:, :early], wo_s[:early, here], 1, 0)
    pair_all(wo_s, n - EARLY, 3).wait_recv()
    for i in range(dim // wide):
        here = slice(i * wide, (i + 1) * wide)
        y_ref[:, here] = (early_s[:, here] + _dot(a_s[:, early:], wo_s[early:, here], 1, 0)).astype(jnp.bfloat16)

    for name, ref in (("w", w_s), ("wo", wo_s)):
        for c in range(2):
            rows = ref.at[pl.ds(0, (n - 1) * chunk), :]
            pltpu.make_async_remote_copy(rows, rows, send_sem.at[gathers[name][2] + c], w_recv.at[0, 0], device_id={"sp": up1},
                                         device_id_type=MESH).wait_send()
    rows = k_s.at[pl.ds(0, (n - 1) * own), :]
    pltpu.make_async_remote_copy(rows, rows, send_sem.at[4], w_recv.at[0, 0], device_id={"sp": up1}, device_id_type=MESH).wait_send()
    rows = vt_s.at[pl.ds(0, n - 1)]
    pltpu.make_async_remote_copy(rows, rows, send_sem.at[5], w_recv.at[0, 0], device_id={"sp": up1}, device_id_type=MESH).wait_send()
    pair_all(w_s, EARLY - 1, 0).wait_send()
    pair_all(w_s, n - EARLY, 1).wait_send()
    pair_all(wo_s, EARLY - 1, 2).wait_send()
    pair_all(wo_s, n - EARLY, 3).wait_send()


def solution(mesh):
    n = mesh.shape["sp"]
    side = math.isqrt(n)

    def step(x, gain, wq, wk, wv, wo):
        own, dim = x.shape
        shard, qd = wq.shape
        kd = wk.shape[1]
        heads, half = qd // HEAD, HEAD // 2
        freq = jnp.asarray((THETA ** (-np.arange(half) / half))[None].astype(np.float32))
        low, wide = jnp.bfloat16, jnp.float32
        dma = pltpu.SemaphoreType.DMA
        anywhere, vmem = pl.BlockSpec(memory_space=pl.ANY), pl.BlockSpec(memory_space=pltpu.VMEM)
        return pl.pallas_call(
            functools.partial(_kernel, side),
            out_shape=pltpu.VMEM((own, dim), low),
            in_specs=[anywhere, vmem, vmem, anywhere, anywhere, anywhere, anywhere],
            out_specs=vmem,
            scratch_shapes=[
                pltpu.VMEM((own, dim), low),
                pltpu.VMEM((own, dim), low),
                pltpu.VMEM((n * shard, qd + 2 * kd), low),
                pltpu.VMEM((n * wo.shape[0], wo.shape[1]), low),
                pltpu.VMEM((n * own, HEAD), low),
                pltpu.VMEM((n, HEAD, own), low),
                pltpu.VMEM((HEAD, heads * own), low),
                pltpu.VMEM((HEAD + 8, heads * own), wide),
                pltpu.VMEM((1, heads * own), wide),
                pltpu.VMEM((own, half), wide),
                pltpu.VMEM((own, half), wide),
                pltpu.VMEM((own, qd + 2 * kd), wide),
                dma((5,)),
                dma((n, 2)),
                dma((n, 2)),
                dma((n, 2)),
                dma((4,)),
                dma((6,)),
                dma((4,)),
            ],
            compiler_params=pltpu.CompilerParams(collective_id=0, has_side_effects=True, vmem_limit_bytes=VMEM - 2 * own * dim),
        )(x, gain, freq, wq, wk, wv, wo)

    tokens, whole = P(("dp", "sp"), None), P("sp", None)
    return jax.shard_map(
        step,
        mesh=mesh,
        in_specs=(tokens, P(None), whole, whole, whole, whole),
        out_specs=tokens,
        check_vma=False,
    )
```

```python
import functools
import math

import jax
import jax.numpy as jnp
import numpy as np
from jax import lax
from jax.experimental import pallas as pl
from jax.experimental.pallas import tpu as pltpu
from jax.sharding import PartitionSpec as P

HEAD = 256
THETA = 10000
NEG = -1e30
HIDDEN = 2 * NEG
LOG2E = 1.4426950408889634
VMEM = 67_043_328
EARLY = 9
AHEAD = 0
AHEAD_WO = 13
MESH = pl.DeviceIdType.MESH


def _dot(a, b, ca, cb):
    return lax.dot_general(a, b, (((ca,), (cb,)), ((), ())), preferred_element_type=jnp.float32)


def _gray(i):
    return jnp.where(i >= 2, 5 - i, i)


def _turn(t):
    t = jnp.int32(t)
    t = jnp.where((t >= 3) & (t <= 5), jnp.where(t == 5, 3, t + 1), t)
    near = (t >= 4) & (t < 12)
    df = _gray(jnp.where(near, lax.div(t - 4, 2), lax.rem(t, 4)))
    return df, jnp.where(near, 1 + 2 * lax.rem(t, 2), jnp.where(t >= 12, 2, 0))


def _kernel(side, x_hbm, gain_ref, freq_ref, wq_hbm, wk_hbm, wv_hbm, wo_hbm, y_ref, x_s, a_s, w_s, wo_s, k_s, vt_s, qt_s, mix_s, top_s, cos_s,
            sin_s, early_s, local_sem, w_recv, wo_recv, kv_recv, pair_recv, send_sem, pair_send):
    n = side * side
    own, dim = x_hbm.shape
    shard = wq_hbm.shape[0]
    part, chunk = shard // 2, shard // 4
    qd = wq_hbm.shape[1]
    heads = qd // HEAD
    half = HEAD // 2
    e = HEAD**-0.5 * LOG2E

    me = lax.axis_index("sp")
    group = lax.axis_index("dp")
    odd = group % 2
    partner = group + 1 - 2 * odd
    px, py = me // side, me % side
    first = px * (1 - odd) + py * odd
    second = py * (1 - odd) + px * odd

    by_first, by_second = side * (1 - odd) + odd, side * odd + 1 - odd

    def place(f, s):
        f, s = lax.rem(f + side, side), lax.rem(s + side, side)
        return f * by_first + s * by_second

    def source(df, ds):
        return place(first - df, second - ds)

    up1, down1 = place(first + 1, second), place(first - 1, second)
    up2, down2 = place(first, second + 1), place(first, second - 1)

    def slot(df, ds):
        dx, dy = jnp.where(odd == 1, ds, df), jnp.where(odd == 1, df, ds)
        gx, gy = jnp.minimum(dx, 2), jnp.minimum(dy, 2)
        return jnp.where(dx == 2, EARLY + dy, jnp.where(dy == 2, EARLY + side + gx, gx * (side - 1) + gy))

    def w_chunk(src, c, df, ds):
        return w_s.at[pl.ds(pl.multiple_of(slot(df, ds) * shard + odd * part + c * chunk, chunk), chunk), :]

    def wo_chunk(src, c, df, ds):
        return wo_s.at[pl.ds(pl.multiple_of(slot(df, ds) * shard + odd * part + c * chunk, chunk), chunk), :]

    def kv_chunk(src, c, df, ds):
        return k_s.at[pl.ds(pl.multiple_of(src * own, own), own), :] if c == 0 else vt_s.at[src]

    gathers = {"w": (w_chunk, w_recv, 0), "wo": (wo_chunk, wo_recv, 2), "kv": (kv_chunk, kv_recv, 4)}

    def send(name, src, c, target, here, there):
        at, recv, sem = gathers[name]
        df, ds = there
        pltpu.make_async_remote_copy(at(src, c, *here), at(src, c, df, ds), send_sem.at[sem + c], recv.at[df * side + ds, c],
                                     device_id={"sp": target}, device_id_type=MESH).start()

    def start_first(name):
        for c in range(2):
            send(name, me, c, up1, (0, 0), (1, 0))
            send(name, me, c, down1, (0, 0), (side - 1, 0))

    def start_second(name):
        for c in range(2):
            send(name, me, c, up2, (0, 0), (0, 1))
            send(name, me, c, down2, (0, 0), (0, side - 1))

    def pair_copy(rows, i):
        return pltpu.make_async_remote_copy(rows, rows, pair_send.at[i], pair_recv.at[i], device_id={"dp": partner}, device_id_type=MESH)

    def pair_w(ref, place, i):
        return pair_copy(ref.at[pl.ds(pl.multiple_of(place * shard + odd * part, part), part), :], i)

    def pair_all(ref, blocks, i):
        return pair_copy(ref.at[pl.ds(0, blocks * part), :], i)

    def relay(name, t):
        df, ds = here = _turn(t)
        src = source(df, ds)
        at, recv, sem = gathers[name]
        for c in range(2):
            ref = at(src, c, df, ds)
            pltpu.make_async_remote_copy(ref, ref, send_sem.at[sem + c], recv.at[df * side + ds, c], device_id={"sp": up1},
                                         device_id_type=MESH).wait_recv()
            turn, on1, on2 = (1, up1, up2) if c == 0 else (side - 1, down1, down2)

            @pl.when(ds == 0)
            def _():
                @pl.when(df == turn)
                def _():
                    send(name, src, c, on1, here, (2, 0))

                send(name, src, c, up2, here, (df, 1))
                send(name, src, c, down2, here, (df, side - 1))

            @pl.when(ds == turn)
            def _():
                send(name, src, c, on2, here, (df, 2))

        if name != "kv":
            ref, i = (w_s, 0) if name == "w" else (wo_s, 2)
            far = (df == 2) | (ds == 2)

            @pl.when(far)
            def _():
                pair_w(ref, slot(df, ds), i + 1).start()

            @pl.when(jnp.logical_not(far))
            def _():
                pair_w(ref, slot(df, ds), i).start()

        return src

    top = pl.ds(0, shard)
    kd = wk_hbm.shape[1]
    copies = [
        pltpu.make_async_copy(wq_hbm, w_s.at[top, pl.ds(0, qd)], local_sem.at[0]),
        pltpu.make_async_copy(wk_hbm, w_s.at[top, pl.ds(qd, kd)], local_sem.at[1]),
        pltpu.make_async_copy(wv_hbm, w_s.at[top, pl.ds(qd + kd, kd)], local_sem.at[2]),
        pltpu.make_async_copy(x_hbm, x_s, local_sem.at[3]),
        pltpu.make_async_copy(wo_hbm, wo_s.at[top, :], local_sem.at[4]),
    ]
    for copy in copies[:3]:
        copy.start()

    barrier = pltpu.get_barrier_semaphore()
    for target in (up1, down1, up2, down2):
        pl.semaphore_signal(barrier, inc=1, device_id={"sp": target}, device_id_type=MESH)
    pl.semaphore_signal(barrier, inc=1, device_id={"dp": partner}, device_id_type=MESH)
    for copy in copies[:3]:
        copy.wait()
    pl.semaphore_wait(barrier, 5)
    start_first("w")
    start_second("w")
    for copy in copies[3:]:
        copy.start()
    for t in range(1, side):
        relay("w", t)

    def columns_of(i):
        dx, dy = (px - i // side + side) % side, (py - i % side + side) % side
        return pl.ds(pl.multiple_of(slot(dx * (1 - odd) + dy * odd, dy * (1 - odd) + dx * odd) * shard, shard), shard)

    copies[3].wait()
    gain = gain_ref[...].astype(jnp.float32).reshape(1, dim)
    rows = own // side

    def prepare(t, _):
        relay("w", t)
        at = pl.multiple_of((t - side) * rows, rows)
        here = pl.ds(at, rows)
        wide = x_s[here, :].astype(jnp.float32)
        scale = lax.rsqrt(jnp.mean(wide * wide, -1, keepdims=True) + 1e-6)
        state = (wide * scale * gain).astype(jnp.bfloat16)
        for i in range(n):
            a_s[here, columns_of(i)] = state[:, i * shard : (i + 1) * shard]
        where = (me * own + at + lax.broadcasted_iota(jnp.int32, (rows, half), 0)).astype(jnp.float32)
        angle = where * freq_ref[...]
        cos_s[here, :] = jnp.cos(angle)
        sin_s[here, :] = jnp.sin(angle)

    lax.fori_loop(side, 2 * side, prepare, None)
    copies[4].wait()
    start_first("wo")
    start_second("wo")
    top_s[...] = jnp.full(top_s.shape, NEG, jnp.float32)
    mix_s[...] = jnp.zeros(mix_s.shape, jnp.float32)
    lax.fori_loop(2 * side, n - side, lambda t, _: (relay("w", t), None)[1], None)

    early = EARLY * shard

    def columns(at):
        return pl.ds(pl.multiple_of(at, HEAD), HEAD)

    def project_early(i):
        at = columns(i * HEAD)
        early_s[:, at] = _dot(a_s[:, :early], w_s[:early, at], 1, 0)

    pair_all(w_s, EARLY - 1, 0).wait_recv()
    pieces = (qd + 2 * kd) // HEAD

    def rest(t, _):
        for i in range(-(-pieces // side)):
            at = (t - n + side) * -(-pieces // side) + i

            @pl.when(at < pieces)
            def _():
                project_early(at)

        relay("w", t)

    lax.fori_loop(n - side, n, rest, None)
    pair_all(w_s, n - EARLY, 1).wait_recv()

    def project(at):
        at = columns(at)
        return (early_s[:, at] + _dot(a_s[:, early:], w_s[early:, at], 1, 0)).astype(jnp.bfloat16)

    def turned(t):
        a, b = t[:, :half].astype(jnp.float32), t[:, half:].astype(jnp.float32)
        cos, sin = cos_s[...], sin_s[...]
        return jnp.concatenate([a * cos - b * sin, b * cos + a * sin], -1)

    k_s[pl.ds(pl.multiple_of(me * own, own), own), :] = turned(project(qd)).astype(jnp.bfloat16)
    vt_s[me] = project(qd + kd).astype(jnp.float32).T.astype(jnp.bfloat16)

    def query(h):
        qt_s[:, pl.ds(pl.multiple_of(h * own, own), own)] = turned(project(h * HEAD)).T.astype(jnp.bfloat16)

    query(0)
    start_first("kv")

    lax.fori_loop(1, heads // 2, lambda h, _: query(h), None)
    relay("wo", 1)
    lax.fori_loop(heads // 2, heads, lambda h, _: query(h), None)
    start_second("kv")

    ones = jnp.ones((8, own), jnp.bfloat16)

    def block(j, masked):
        keys = k_s[pl.ds(pl.multiple_of(j * own, own), own), :]
        values = jnp.concatenate([vt_s[j], ones], axis=0)
        if masked:
            ok = lax.broadcasted_iota(jnp.int32, (own, own), 1) >= lax.broadcasted_iota(jnp.int32, (own, own), 0)

        def score(h):
            return _dot(keys, qt_s[:, h * own : (h + 1) * own], 1, 0)

        def weigh(h, s):
            here = slice(h * own, (h + 1) * own)
            if masked:
                s = jnp.where(ok, s, HIDDEN)
            old = top_s[:, here]
            top = jnp.maximum(old, s.max(axis=0, keepdims=True))
            top_s[:, here] = top
            return jnp.exp2((s - top) * e).astype(jnp.bfloat16), jnp.exp2((old - top) * e)

        def mix(h, p, keep):
            here = slice(h * own, (h + 1) * own)
            mix_s[:, here] = mix_s[:, here] * keep + _dot(values, p, 1, 0)

        scores = [score(0), score(1)]
        last = None
        for h in range(heads):
            if h + 2 < heads:
                scores.append(score(h + 2))
            now = weigh(h, scores[h])
            if last is not None:
                mix(h - 1, *last)
            last = now
        mix(heads - 1, *last)

    block(me, True)
    for t in range(1, AHEAD + 1):
        relay("kv", t)

    def attend(t, _):
        @pl.when(t < n - AHEAD)
        def _():
            relay("kv", t + AHEAD)

        @pl.when((t >= side) & (t < n - 1))
        def _():
            relay("wo", t - side + 2)

        src = source(*_turn(t))

        @pl.when(src < me)
        def _():
            block(src, False)

    lax.fori_loop(1, n, attend, None)

    for h in range(heads):
        here = slice(h * own, (h + 1) * own)
        seen = (mix_s[:HEAD, here] * (1 / mix_s[HEAD : HEAD + 1, here])).T.astype(jnp.bfloat16)
        for i in range(HEAD // shard):
            a_s[:, columns_of(h * (HEAD // shard) + i)] = seen[:, i * shard : (i + 1) * shard]

    for t in range(AHEAD_WO, n):
        relay("wo", t)
    pair_all(wo_s, EARLY - 1, 2).wait_recv()
    wide = 512
    for i in range(dim // wide):
        here = slice(i * wide, (i + 1) * wide)
        early_s[:, here] = x_s[:, here].astype(jnp.float32) + _dot(a_s[:, :early], wo_s[:early, here], 1, 0)
    pair_all(wo_s, n - EARLY, 3).wait_recv()
    for i in range(dim // wide):
        here = slice(i * wide, (i + 1) * wide)
        y_ref[:, here] = (early_s[:, here] + _dot(a_s[:, early:], wo_s[early:, here], 1, 0)).astype(jnp.bfloat16)

    for name, ref in (("w", w_s), ("wo", wo_s)):
        for c in range(2):
            rows = ref.at[pl.ds(0, (n - 1) * chunk), :]
            pltpu.make_async_remote_copy(rows, rows, send_sem.at[gathers[name][2] + c], w_recv.at[0, 0], device_id={"sp": up1},
                                         device_id_type=MESH).wait_send()
    rows = k_s.at[pl.ds(0, (n - 1) * own), :]
    pltpu.make_async_remote_copy(rows, rows, send_sem.at[4], w_recv.at[0, 0], device_id={"sp": up1}, device_id_type=MESH).wait_send()
    rows = vt_s.at[pl.ds(0, n - 1)]
    pltpu.make_async_remote_copy(rows, rows, send_sem.at[5], w_recv.at[0, 0], device_id={"sp": up1}, device_id_type=MESH).wait_send()
    pair_all(w_s, EARLY - 1, 0).wait_send()
    pair_all(w_s, n - EARLY, 1).wait_send()
    pair_all(wo_s, EARLY - 1, 2).wait_send()
    pair_all(wo_s, n - EARLY, 3).wait_send()


def solution(mesh):
    n = mesh.shape["sp"]
    side = math.isqrt(n)

    def step(x, gain, wq, wk, wv, wo):
        own, dim = x.shape
        shard, qd = wq.shape
        kd = wk.shape[1]
        heads, half = qd // HEAD, HEAD // 2
        freq = jnp.asarray((THETA ** (-np.arange(half) / half))[None].astype(np.float32))
        low, wide = jnp.bfloat16, jnp.float32
        dma = pltpu.SemaphoreType.DMA
        anywhere, vmem = pl.BlockSpec(memory_space=pl.ANY), pl.BlockSpec(memory_space=pltpu.VMEM)
        return pl.pallas_call(
            functools.partial(_kernel, side),
            out_shape=pltpu.VMEM((own, dim), low),
            in_specs=[anywhere, vmem, vmem, anywhere, anywhere, anywhere, anywhere],
            out_specs=vmem,
            scratch_shapes=[
                pltpu.VMEM((own, dim), low),
                pltpu.VMEM((own, dim), low),
                pltpu.VMEM((n * shard, qd + 2 * kd), low),
                pltpu.VMEM((n * wo.shape[0], wo.shape[1]), low),
                pltpu.VMEM((n * own, HEAD), low),
                pltpu.VMEM((n, HEAD, own), low),
                pltpu.VMEM((HEAD, heads * own), low),
                pltpu.VMEM((HEAD + 8, heads * own), wide),
                pltpu.VMEM((1, heads * own), wide),
                pltpu.VMEM((own, half), wide),
                pltpu.VMEM((own, half), wide),
                pltpu.VMEM((own, qd + 2 * kd), wide),
                dma((5,)),
                dma((n, 2)),
                dma((n, 2)),
                dma((n, 2)),
                dma((4,)),
                dma((6,)),
                dma((4,)),
            ],
            compiler_params=pltpu.CompilerParams(collective_id=0, has_side_effects=True, vmem_limit_bytes=VMEM - 2 * own * dim),
        )(x, gain, freq, wq, wk, wv, wo)

    tokens, whole = P(("dp", "sp"), None), P("sp", None)
    return jax.shard_map(
        step,
        mesh=mesh,
        in_specs=(tokens, P(None), whole, whole, whole, whole),
        out_specs=tokens,
        check_vma=False,
    )
```
